32 devices in a mesh: grp: 4 (over y, x), zero: 8 (over z, core).
Axes of the slice: x: 2, y: 2, z: 4, core: 2. Of those that a mesh axis runs over, the one named last changes fastest.
Arguments:
- replica_grads: bfloat16 [4, 3072, 2, 12288], P('grp', None, None, 'zero'), may hold values from -20000 to 20000, as said below
- master_weights: float32 [3072, 2, 12288], P(('grp', 'zero')), may hold values from -0.6 to 0.6
- first_moment: float32 [3072, 2, 12288], P(('grp', 'zero')), may hold values from -0.3 to 0.3
- second_moment: float32 [3072, 2, 12288], P(('grp', 'zero')), may hold values from 0.001 to 0.03
- max_norm: float32 [1], replicated, may hold values from 1737.7856 to 4344.464
Outputs:
- new_master: float32 [3072, 2, 12288], P(('grp', 'zero'))
- new_first: float32 [3072, 2, 12288], P(('grp', 'zero'))
- new_second: float32 [3072, 2, 12288], P(('grp', 'zero'))
- new_weights: bfloat16 [3072, 2, 12288], P(None, None, 'zero')
The draws below stay inside these ranges and needn't reach their ends.
Inputs may be any that keep to these rules, and one draw needn't show every extreme that they name: `replica_grads`: one gradient of the joined weight for each replica group.
All inputs are finite; a program needn't handle non-finite values.
Results may differ from the reference program's by a relative error of at most 0.015.
Values may be sent and summed in bfloat16 or wider, within the bound.
A program may use at most 192 MiB of HBM per device.

```python
import math
import jax
import jax.numpy as jnp

D = 3072
FF = 12288
ADAM_STEP = 10
N_GRP = 4


def draw_replica_grads(key, part):
    first_key, second_key, third_key, fourth_key, fifth_key = jax.random.split(key, 5)
    log_top = math.log(10.0)
    row_index = jnp.arange(D, dtype=jnp.float32)
    column_index = jnp.arange(FF, dtype=jnp.float32)
    row_scale = jnp.sqrt(1.0 + 2.0 * row_index / (D - 1)) * jnp.exp(jax.random.uniform(first_key, (D,), jnp.float32) * log_top)
    column_scale = jnp.sqrt(1.0 + 2.0 * column_index / (FF - 1))[None, :] * jnp.exp(jax.random.uniform(second_key, (2, FF), jnp.float32) * log_top)
    levels = jnp.arange(N_GRP, dtype=jnp.float32) / max(N_GRP - 1, 1)
    band_mix = jax.random.permutation(fifth_key, levels)
    row_mix = jnp.repeat(band_mix, D // N_GRP, total_repeat_length=D)
    replica_sign = jnp.where(jnp.arange(N_GRP) % 2 == 0, 1.0, -1.0).astype(jnp.float32)
    common_weight = row_mix[None, :] + (1.0 - row_mix[None, :]) * replica_sign[:, None]
    independent = jax.random.truncated_normal(third_key, -4.0, 4.0, (N_GRP, D, 2, FF), jnp.float32)
    common = jax.random.truncated_normal(fourth_key, -4.0, 4.0, (D, 2, FF), jnp.float32)
    random_part = 0.5 * independent + common_weight[:, :, None, None] * common[None]
    values = random_part * row_scale[None, :, None, None] * column_scale[None, None, :, :]
    return values.astype(jnp.bfloat16)


def level_of(rng, shape, pieces, low, top_value):
    factor_of = 1.0
    for dim, blocks in pieces:
        steps = jax.random.uniform(jax.random.fold_in(jax.random.fold_in(rng, 6), dim), (blocks,), jnp.float32, low / len(pieces), top_value / len(pieces))
        factor_of = factor_of * jnp.repeat(jnp.exp(steps), shape[dim] // blocks).reshape((-1,) + (1,) * (len(shape) - 1 - dim))
    return factor_of


def gaussian(key, shape, scale, bound, cuts=(), held_as=jnp.bfloat16):
    values = scale * jax.random.normal(key, shape, jnp.float32)
    if cuts:
        values = values * level_of(key, shape, cuts, -0.22, 0.18)
    return jnp.clip(values, -bound, bound).astype(held_as)


def setup_inputs(seed: int = 0) -> dict:
    splits = jax.random.split(jax.random.key(seed), 6)
    return {
        "replica_grads": draw_replica_grads(jax.random.fold_in(splits[5], 71), 0),
        "master_weights": gaussian(splits[1], (D, 2, FF), 0.1, 0.6, ((0, 32),), jnp.float32),
        "first_moment": gaussian(splits[2], (D, 2, FF), 0.05, 0.3, ((0, 32),), jnp.float32),
        "second_moment": jnp.clip(jnp.exp(math.log(0.03) - 3.4011973 * jax.random.uniform(splits[3], (D, 2, FF), jnp.float32) ** level_of(splits[3], (D, 2, FF), ((0, 32),), -0.2, 0.2)), 0.001, 0.03),
        "max_norm": jnp.clip(jax.random.uniform(splits[4], (1,), jnp.float32, 1737.7856, 4344.464), 1737.7856, 4344.464),
    }


beta_one = 0.9
beta_two = 0.95
learn_rate = 0.02
adam_eps = 1e-08
norm_eps = 1e-06

def adam_update(summed, master, first, second, scale):
    clipped = summed * scale
    new_first = beta_one * first + (1.0 - beta_one) * clipped
    new_second = beta_two * second + (1.0 - beta_two) * clipped * clipped
    correct_one = 1.0 - beta_one ** ADAM_STEP
    correct_two = 1.0 - beta_two ** ADAM_STEP
    step_size = new_first / correct_one / (jnp.sqrt(new_second / correct_two) + adam_eps)
    new_master = master - learn_rate * step_size
    return (new_master, new_first, new_second)

def reference(replica_grads, master_weights, first_moment, second_moment, max_norm):
    summed = replica_grads[0].astype(jnp.float32)
    for replica in range(1, N_GRP):
        summed = summed + replica_grads[replica].astype(jnp.float32)
    total = jnp.sum(summed * summed)
    scale = jnp.minimum(jnp.float32(1.0), max_norm[0] / (jnp.sqrt(total) + norm_eps))
    new_master, new_first, new_second = adam_update(summed, master_weights, first_moment, second_moment, scale)
    return (new_master, new_first, new_second, new_master.astype(jnp.bfloat16))
```

```python
import functools

import jax
import jax.numpy as jnp
from jax import lax
from jax.experimental import pallas as pl
from jax.experimental.pallas import tpu as pltpu
from jax.experimental.layout import Layout, with_layout_constraint
from jax.sharding import PartitionSpec as P

ADAM_STEP = 10
MESH = pl.DeviceIdType.MESH
LANES = 128

beta_one = 0.9
beta_two = 0.95
learn_rate = 0.02
adam_eps = 1e-08
norm_eps = 1e-06


def adam_update(summed, master, first, second, scale):
    clipped = summed * scale
    new_first = beta_one * first + (1.0 - beta_one) * clipped
    new_second = beta_two * second + (1.0 - beta_two) * clipped * clipped
    correct_one = 1.0 - beta_one**ADAM_STEP
    correct_two = 1.0 - beta_two**ADAM_STEP
    step_size = new_first / correct_one / (jnp.sqrt(new_second / correct_two) + adam_eps)
    new_master = master - learn_rate * step_size
    return (new_master, new_first, new_second)


def plain_body(replica_grads, master_weights, first_moment, second_moment, max_norm):
    groups = lax.axis_size("grp")
    shards = lax.axis_size("zero")
    local_grad = replica_grads[0]
    local_width = local_grad.shape[2]
    rows_dev = master_weights.shape[0]
    full_width = master_weights.shape[2]
    blocks = local_grad.reshape(groups, shards, rows_dev, 2, local_width)
    arrived = lax.all_to_all(
        lax.all_to_all(blocks[None], "grp", split_axis=1, concat_axis=0, tiled=True),
        "zero",
        split_axis=2,
        concat_axis=5,
        tiled=True,
    )
    summed = jnp.sum(arrived.astype(jnp.float32), axis=0)
    summed = summed.reshape(master_weights.shape)
    total = lax.psum(jnp.sum(summed * summed), ("grp", "zero"))
    scale = jnp.minimum(jnp.float32(1.0), max_norm[0] / (jnp.sqrt(total) + norm_eps))
    new_master, new_first, new_second = adam_update(
        summed, master_weights, first_moment, second_moment, scale
    )
    fresh = new_master.astype(jnp.bfloat16).reshape(1, 1, rows_dev, 2, full_width)
    own_tiles = lax.all_to_all(fresh, "zero", split_axis=4, concat_axis=1, tiled=True)
    tiled = lax.all_gather(own_tiles, "grp", axis=0, tiled=True)
    new_weights = tiled.reshape(groups * shards * rows_dev, 2, full_width // shards)
    return (new_master, new_first, new_second, new_weights)


def flip(index, mask, size):
    out = 0
    bit = 1
    while bit < size:
        b = (index // bit) % 2
        out = out + bit * ((1 - b) if mask & bit else b)
        bit *= 2
    return out


def greet(groups, shards, g, z):
    barrier = pltpu.get_barrier_semaphore()
    for k in range(1, shards):
        pl.semaphore_signal(barrier, inc=1, device_id=(g, flip(z, k, shards)), device_id_type=MESH)
    for j in range(1, groups):
        pl.semaphore_signal(barrier, inc=1, device_id=(flip(g, j, groups), z), device_id_type=MESH)
    pl.semaphore_wait(barrier, shards + groups - 2)


def remote(src, dst, send, recv, device):
    return pltpu.make_async_remote_copy(
        src_ref=src, dst_ref=dst, send_sem=send, recv_sem=recv,
        device_id=device, device_id_type=MESH,
    )


def step_kernel(groups, shards, limit, grad, master_in, first_in, second_in, master, first, second, out,
                sums, landed, zone, gone, f_send, f_recv, load_sem, p_send, p_recv, s_send, s_recv,
                nz_send, nz_recv, ng_send, ng_recv, state_sem, z_send, z_recv, x_send, x_recv, y_send, y_recv,
                u_send, u_recv, v_send, v_recv):
    g, z = lax.axis_index("grp"), lax.axis_index("zero")
    gx, gy, diagonal = flip(g, 1, groups), flip(g, 2, groups), flip(g, 3, groups)
    first_to, second_to = (gx, gy), (gy, gx)
    rows = landed.shape[1]
    half = rows // 2
    order = list(range(shards - 1, -1, -1))
    near, far, got, pairs = (out.at[i] for i in range(4))
    bf16, f32 = jnp.bfloat16, jnp.float32

    def part(ref, k, h):
        return ref.at[k, pl.ds(h * half, half)]

    def raw(k, h, d):
        block = diagonal if d else first_to[h]
        return remote(grad.at[block, flip(z, k, shards), h], part(far if d else near, k, h),
                      f_send.at[k, h, d], f_recv.at[k, h, d], (first_to[h], z))

    def pair(k, h):
        return remote(part(pairs, k, h), part(got, k, h), p_send.at[k, h], p_recv.at[k, h], (second_to[h], z))

    def load(k, h, d):
        block = second_to[h] if d else g
        return pltpu.make_async_copy(grad.at[block, flip(z, k, shards), h], part(pairs if d else sums, k, h),
                                     load_sem.at[k, h, d])

    def onward(k):
        return remote(sums.at[k], landed.at[z], s_send.at[k], s_recv.at[k], (g, flip(z, k, shards)))

    states = [
        pltpu.make_async_copy(src, dst, state_sem.at[i])
        for i, (src, dst) in enumerate(((master_in, master), (first_in, first), (second_in, second)))
    ]

    greet(groups, shards, g, z)
    ahead = 2
    for k in order[:ahead]:
        for h in (0, 1):
            raw(k, h, 1).start()
    for k in order:
        for d in (1, 0):
            for h in (0, 1):
                load(k, h, d).start()
    for state in states:
        state.start()
    square = jnp.zeros(landed.shape[2:], f32)
    for i in range(shards + 1):
        if i < shards:
            k = order[i]
            for h in (0, 1):
                load(k, h, 1).wait()
                raw(k, h, 1).wait_recv()

                def join(r, carry, k=k, h=h):
                    row = h * half + r
                    both = pairs[k, row].astype(f32) + far[k, row].astype(f32)
                    pairs[k, row] = both.astype(bf16)
                    return carry

                lax.fori_loop(0, half, join, 0)
                pair(k, h).start()
            for h in (0, 1):
                raw(k, h, 0).start()
            if i + ahead < shards:
                for h in (0, 1):
                    raw(order[i + ahead], h, 1).start()
        if i >= 1:
            k = order[i - 1]
            for h in (0, 1):
                load(k, h, 0).wait()
                raw(k, h, 0).wait_recv()
                pair(k, h).wait_recv()

                def add(r, acc, k=k, h=h):
                    row = h * half + r
                    total = sums[k, row].astype(f32) + near[k, row].astype(f32)
                    total = total + got[k, row].astype(f32)
                    if k:
                        sums[k, row] = total.astype(bf16)
                    else:
                        landed[z, row] = total.astype(bf16)
                    return acc + total * total

                square = lax.fori_loop(0, half, add, square)
            if k:
                onward(k).start()

    folded = square[0:8]
    for i in range(8, square.shape[0], 8):
        folded = folded + square[i:i + 8]
    zone[0] = folded

    def tell_zero(k):
        return remote(zone.at[0], zone.at[k], nz_send.at[k], nz_recv.at[k], (g, flip(z, k, shards)))

    def tell_group(j):
        return remote(gone.at[0], gone.at[j], ng_send.at[j], ng_recv.at[j], (flip(g, j, groups), z))

    for k in order:
        for h in (0, 1):
            pair(k, h).wait_send()
    for k in range(1, shards):
        tell_zero(k).start()
    for k in range(1, shards):
        tell_zero(k).wait_recv()
    gone[0] = jnp.sum(zone[...], axis=0)
    for j in range(1, groups):
        tell_group(j).start()
    for j in range(1, groups):
        tell_group(j).wait_recv()
    norm = jnp.sum(gone[...], axis=0)
    total = jnp.full(landed.shape[2:], jnp.sum(norm), f32)
    scale = jnp.minimum(f32(1.0), limit[0] / (jnp.sqrt(total) + norm_eps))
    rate_one = learn_rate / (1.0 - beta_one**ADAM_STEP)
    over_two = 1.0 / (1.0 - beta_two**ADAM_STEP)

    def update(k):
        c = flip(z, k, shards)

        def row(r, carry):
            clipped = landed[c, r].astype(f32) * scale
            new_first = beta_one * first[r, c] + (1.0 - beta_one) * clipped
            new_second = beta_two * second[r, c] + (1.0 - beta_two) * clipped * clipped
            below = jnp.sqrt(new_second * over_two) + adam_eps
            new_master = master[r, c] - new_first * rate_one / below
            master[r, c] = new_master
            first[r, c] = new_first
            second[r, c] = new_second
            if k:
                landed[c, r] = new_master.astype(bf16)
            else:
                out[g, z, r] = new_master.astype(bf16)
            return carry

        lax.fori_loop(0, rows, row, 0)

    def spread(k):
        return remote(landed.at[flip(z, k, shards)], out.at[g, z], z_send.at[k], z_recv.at[k],
                      (g, flip(z, k, shards)))

    def first_hop(k, send, recv, to):
        ref = out.at[g, flip(z, k, shards)]
        return remote(ref, ref, send.at[k], recv.at[k], (to, z))

    def second_hop(k, origin, start, send, recv, to):
        ref = out.at[origin, flip(z, k, shards), pl.ds(start, half)]
        return remote(ref, ref, send.at[k], recv.at[k], (to, z))

    def hops(k):
        return (first_hop(k, x_send, x_recv, gx), first_hop(k, y_send, y_recv, gy))

    def turns(k):
        return (second_hop(k, gx, 0, u_send, u_recv, gy), second_hop(k, gy, half, v_send, v_recv, gx))

    for state in states:
        state.wait()
    update(0)
    for hop in hops(0):
        hop.start()
    for k in range(1, shards):
        onward(k).wait_recv()
        update(k)
        spread(k).start()
    lag = 1
    for s in range(1, shards + lag):
        if s < shards:
            spread(s).wait_recv()
            for hop in hops(s):
                hop.start()
        if s >= lag:
            for hop, turn in zip(hops(s - lag), turns(s - lag)):
                hop.wait_recv()
                turn.start()
    for k in range(1, shards):
        tell_zero(k).wait_send()
        onward(k).wait_send()
        spread(k).wait_send()
    for j in range(1, groups):
        tell_group(j).wait_send()
    for k in order:
        for h in (0, 1):
            for d in (0, 1):
                raw(k, h, d).wait_send()
        for hop in hops(k):
            hop.wait_send()
        for turn in turns(k):
            turn.wait()


def store_kernel(pieces, *refs):
    count = len(refs) // 2
    sources, targets, sem = refs[:count], refs[count:2 * count], refs[-1]
    copies = []
    for i, (source, target) in enumerate(zip(sources, targets)):
        size = source.shape[0] // pieces
        for j in range(pieces):
            span = pl.ds(j * size, size)
            copies.append(pltpu.make_async_copy(source.at[span], target.at[span], sem.at[i, j]))
    for copy in copies:
        copy.start()
    for copy in copies:
        copy.wait()


def flat_body(replica_grads, master_weights, first_moment, second_moment, max_norm):
    groups = lax.axis_size("grp")
    shards = lax.axis_size("zero")
    rows = master_weights.shape[0]
    width = replica_grads.shape[3]
    tiles = width // LANES
    deep = 2 * tiles
    bf16, f32 = jnp.bfloat16, jnp.float32
    any_space = pl.BlockSpec(memory_space=pl.ANY)
    vmem = pl.BlockSpec(memory_space=pltpu.VMEM)
    dma = pltpu.SemaphoreType.DMA

    def keep(x, *order):
        return with_layout_constraint(x, Layout(major_to_minor=order))

    def flat(x):
        x = x.reshape(x.shape[0], 2, -1, LANES)
        return jnp.swapaxes(keep(x, 0, 2, 1, 3), 1, 2)

    grad = flat(replica_grads[0]).reshape(groups, shards, 2, rows // 2, deep, LANES)
    master, first, second = (
        flat(x).reshape(rows, shards, deep, LANES)
        for x in (master_weights, first_moment, second_moment)
    )

    block = (shards, rows, deep, LANES)
    state = (rows, shards, deep, LANES)
    grant = 4 * shards * rows * deep * LANES + 192 * 1024
    results = pl.pallas_call(
        functools.partial(step_kernel, groups, shards),
        out_shape=(*[pltpu.VMEM(state, f32)] * 3, pltpu.VMEM((groups,) + block, bf16)),
        in_specs=[pl.BlockSpec(memory_space=pltpu.SMEM)] + [any_space] * 4,
        out_specs=(vmem,) * 4,
        scratch_shapes=[
            *[pltpu.VMEM(block, bf16)] * 2,
            pltpu.VMEM((shards, 8, LANES), f32),
            pltpu.VMEM((groups, 8, LANES), f32),
            *[dma((shards, 2, 2))] * 3,
            *[dma((shards, 2))] * 2,
            *[dma((shards,))] * 4,
            *[dma((groups,))] * 2,
            dma((3,)),
            *[dma((shards,))] * 10,
        ],
        compiler_params=pltpu.CompilerParams(
            collective_id=0, has_side_effects=True, vmem_limit_bytes=grant
        ),
    )(max_norm, grad, master, first, second)

    pieces = 4
    *states, gathered = results
    new_master, new_first, new_second = pl.pallas_call(
        functools.partial(store_kernel, pieces),
        out_shape=(
            *[jax.ShapeDtypeStruct(state, f32)] * 3,
        ),
        in_specs=[any_space] * 3,
        out_specs=(any_space,) * 3,
        scratch_shapes=[dma((3, pieces))],
        compiler_params=pltpu.CompilerParams(vmem_limit_bytes=grant),
    )(*states)

    def unflat(x, shape):
        x = x.reshape(shape[0], -1, 2, LANES)
        return keep(jnp.swapaxes(x, 1, 2), 0, 2, 1, 3).reshape(shape)

    shape = master_weights.shape
    return (
        unflat(new_master, shape),
        unflat(new_first, shape),
        unflat(new_second, shape),
        unflat(gathered, replica_grads.shape[1:]),
    )


def body(replica_grads, master_weights, first_moment, second_moment, max_norm):
    groups = lax.axis_size("grp")
    shards = lax.axis_size("zero")
    rows = master_weights.shape[0]
    width = replica_grads.shape[3]
    deep = 2 * width // LANES
    power = shards > 1 and shards & (shards - 1) == 0
    fits = shards * rows * deep * LANES * (2 * groups + 12 + 4) < 63 * 1024 * 1024
    whole = width % LANES == 0 and deep % 8 == 0 and rows % 2 == 0
    run = flat_body if groups == 4 and power and fits and whole else plain_body
    return run(replica_grads, master_weights, first_moment, second_moment, max_norm)


def solution(mesh):
    in_specs = (
        P("grp", None, None, "zero"),
        P(("grp", "zero"), None, None),
        P(("grp", "zero"), None, None),
        P(("grp", "zero"), None, None),
        P(),
    )
    out_specs = (
        P(("grp", "zero"), None, None),
        P(("grp", "zero"), None, None),
        P(("grp", "zero"), None, None),
        P(None, None, "zero"),
    )
    return jax.shard_map(body, mesh=mesh, in_specs=in_specs, out_specs=out_specs, check_vma=False)
```

```python
import functools

import jax
import jax.numpy as jnp
from jax import lax
from jax.experimental import pallas as pl
from jax.experimental.pallas import tpu as pltpu
from jax.experimental.layout import Layout, with_layout_constraint
from jax.sharding import PartitionSpec as P

ADAM_STEP = 10
MESH = pl.DeviceIdType.MESH
LANES = 128

beta_one = 0.9
beta_two = 0.95
learn_rate = 0.02
adam_eps = 1e-08
norm_eps = 1e-06


def adam_update(summed, master, first, second, scale):
    clipped = summed * scale
    new_first = beta_one * first + (1.0 - beta_one) * clipped
    new_second = beta_two * second + (1.0 - beta_two) * clipped * clipped
    correct_one = 1.0 - beta_one**ADAM_STEP
    correct_two = 1.0 - beta_two**ADAM_STEP
    step_size = new_first / correct_one / (jnp.sqrt(new_second / correct_two) + adam_eps)
    new_master = master - learn_rate * step_size
    return (new_master, new_first, new_second)


def plain_body(replica_grads, master_weights, first_moment, second_moment, max_norm):
    groups = lax.axis_size("grp")
    shards = lax.axis_size("zero")
    local_grad = replica_grads[0]
    local_width = local_grad.shape[2]
    rows_dev = master_weights.shape[0]
    full_width = master_weights.shape[2]
    blocks = local_grad.reshape(groups, shards, rows_dev, 2, local_width)
    arrived = lax.all_to_all(
        lax.all_to_all(blocks[None], "grp", split_axis=1, concat_axis=0, tiled=True),
        "zero",
        split_axis=2,
        concat_axis=5,
        tiled=True,
    )
    summed = jnp.sum(arrived.astype(jnp.float32), axis=0)
    summed = summed.reshape(master_weights.shape)
    total = lax.psum(jnp.sum(summed * summed), ("grp", "zero"))
    scale = jnp.minimum(jnp.float32(1.0), max_norm[0] / (jnp.sqrt(total) + norm_eps))
    new_master, new_first, new_second = adam_update(
        summed, master_weights, first_moment, second_moment, scale
    )
    fresh = new_master.astype(jnp.bfloat16).reshape(1, 1, rows_dev, 2, full_width)
    own_tiles = lax.all_to_all(fresh, "zero", split_axis=4, concat_axis=1, tiled=True)
    tiled = lax.all_gather(own_tiles, "grp", axis=0, tiled=True)
    new_weights = tiled.reshape(groups * shards * rows_dev, 2, full_width // shards)
    return (new_master, new_first, new_second, new_weights)


def flip(index, mask, size):
    out = 0
    bit = 1
    while bit < size:
        b = (index // bit) % 2
        out = out + bit * ((1 - b) if mask & bit else b)
        bit *= 2
    return out


def greet(groups, shards, g, z):
    barrier = pltpu.get_barrier_semaphore()
    for k in range(1, shards):
        pl.semaphore_signal(barrier, inc=1, device_id=(g, flip(z, k, shards)), device_id_type=MESH)
    for j in range(1, groups):
        pl.semaphore_signal(barrier, inc=1, device_id=(flip(g, j, groups), z), device_id_type=MESH)
    pl.semaphore_wait(barrier, shards + groups - 2)


def remote(src, dst, send, recv, device):
    return pltpu.make_async_remote_copy(
        src_ref=src, dst_ref=dst, send_sem=send, recv_sem=recv,
        device_id=device, device_id_type=MESH,
    )


def orders(shards):
    used = [k for k in range(shards) if k != 3 or shards == 4]
    used += [3] * (shards > 4)
    made = [k for k in (shards // 2, 2, shards // 2 + 2, 1) if 0 < k < shards]
    made = list(dict.fromkeys(made + used[1:]))
    return used, made


def partner(z, k, shards):
    low, high = shards // 4, shards // 2
    if low < 2 or k < high:
        return k, flip(z, k, shards)
    one, two = (z // low) % 2, (z // high) % 2
    end = 1 - one - two + 2 * one * two
    return (
        k + end * ((k ^ low) - k),
        flip(z, k, shards) * (1 - end) + flip(z, k ^ low, shards) * end,
    )


def step_kernel(groups, shards, tails, limit, grad, master_in, first_in, second_in, master, first, second, out,
                late_x, late_y, sums, landed, zone, gone, f_send, f_recv, load_sem, p_send, p_recv, s_send, s_recv,
                nz_send, nz_recv, ng_send, ng_recv, state_sem, z_send, z_recv, x_send, x_recv, y_send, y_recv,
                u_send, u_recv, v_send, v_recv):
    g, z = lax.axis_index("grp"), lax.axis_index("zero")
    gx, gy, diagonal = flip(g, 1, groups), flip(g, 2, groups), flip(g, 3, groups)
    first_to, second_to = (gx, gy), (gy, gx)
    rows = landed.shape[1]
    half = rows // 2
    order = list(range(shards - 1, -1, -1))
    used, made = orders(shards)
    late = used[shards - tails:]
    near, far, got, pairs = (out.at[i] for i in range(4))
    bf16, f32 = jnp.bfloat16, jnp.float32

    def part(ref, k, h):
        return ref.at[k, pl.ds(h * half, half)]

    def raw(k, h, d):
        block = diagonal if d else first_to[h]
        return remote(grad.at[block, flip(z, k, shards), h], part(far if d else near, k, h),
                      f_send.at[k, h, d], f_recv.at[k, h, d], (first_to[h], z))

    def pair(k, h):
        return remote(part(pairs, k, h), part(got, k, h), p_send.at[k, h], p_recv.at[k, h], (second_to[h], z))

    def load(k, h, d):
        block = second_to[h] if d else g
        return pltpu.make_async_copy(grad.at[block, flip(z, k, shards), h], part(pairs if d else sums, k, h),
                                     load_sem.at[k, h, d])

    def onward(k):
        return remote(sums.at[k], landed.at[z], s_send.at[k], s_recv.at[k], (g, flip(z, k, shards)))

    states = [
        pltpu.make_async_copy(src, dst, state_sem.at[i])
        for i, (src, dst) in enumerate(((master_in, master), (first_in, first), (second_in, second)))
    ]

    greet(groups, shards, g, z)
    ahead = 2
    for k in order[:ahead]:
        for h in (0, 1):
            raw(k, h, 1).start()
    for k in order:
        for d in (1, 0):
            for h in (0, 1):
                load(k, h, d).start()
    for state in states:
        state.start()
    square = jnp.zeros(landed.shape[2:], f32)
    for i in range(shards + 1):
        if i < shards:
            k = order[i]
            for h in (0, 1):
                load(k, h, 1).wait()
                raw(k, h, 1).wait_recv()

                def join(r, carry, k=k, h=h):
                    row = h * half + r
                    both = pairs[k, row].astype(f32) + far[k, row].astype(f32)
                    pairs[k, row] = both.astype(bf16)
                    return carry

                lax.fori_loop(0, half, join, 0)
                pair(k, h).start()
            for h in (0, 1):
                raw(k, h, 0).start()
            if i + ahead < shards:
                for h in (0, 1):
                    raw(order[i + ahead], h, 1).start()
        if i >= 1:
            k = order[i - 1]
            for h in (0, 1):
                load(k, h, 0).wait()
                raw(k, h, 0).wait_recv()
                pair(k, h).wait_recv()

                def add(r, acc, k=k, h=h):
                    row = h * half + r
                    total = sums[k, row].astype(f32) + near[k, row].astype(f32)
                    total = total + got[k, row].astype(f32)
                    if k:
                        sums[k, row] = total.astype(bf16)
                    else:
                        landed[z, row] = total.astype(bf16)
                    return acc + total * total

                square = lax.fori_loop(0, half, add, square)
            if k:
                onward(k).start()

    folded = square[0:8]
    for i in range(8, square.shape[0], 8):
        folded = folded + square[i:i + 8]
    zone[0] = folded

    def tell_zero(k):
        return remote(zone.at[0], zone.at[k], nz_send.at[k], nz_recv.at[k], (g, flip(z, k, shards)))

    def tell_group(j):
        return remote(gone.at[0], gone.at[j], ng_send.at[j], ng_recv.at[j], (flip(g, j, groups), z))

    for k in order:
        for h in (0, 1):
            pair(k, h).wait_send()
    for k in range(1, shards):
        tell_zero(k).start()
    for k in range(1, shards):
        tell_zero(k).wait_recv()
    gone[0] = jnp.sum(zone[...], axis=0)
    for j in range(1, groups):
        tell_group(j).start()
    for j in range(1, groups):
        tell_group(j).wait_recv()
    norm = jnp.sum(gone[...], axis=0)
    total = jnp.full(landed.shape[2:], jnp.sum(norm), f32)
    scale = jnp.minimum(f32(1.0), limit[0] / (jnp.sqrt(total) + norm_eps))
    rate_one = learn_rate / (1.0 - beta_one**ADAM_STEP)
    over_two = 1.0 / (1.0 - beta_two**ADAM_STEP)

    wide = 4 if half % 4 == 0 else 1

    def update(k, start, count):
        c = flip(z, k, shards)

        def some(i, carry):
            for j in range(wide):
                r = start + i * wide + j
                clipped = landed[c, r].astype(f32) * scale
                new_first = beta_one * first[r, c] + (1.0 - beta_one) * clipped
                new_second = beta_two * second[r, c] + (1.0 - beta_two) * clipped * clipped
                below = jnp.sqrt(new_second * over_two) + adam_eps
                new_master = master[r, c] - new_first * rate_one / below
                master[r, c] = new_master
                first[r, c] = new_first
                second[r, c] = new_second
                if k:
                    landed[c, r] = new_master.astype(bf16)
                else:
                    out[g, z, r] = new_master.astype(bf16)
            return carry

        lax.fori_loop(0, count // wide, some, 0)

    def spread(k):
        return remote(landed.at[flip(z, k, shards)], out.at[g, z], z_send.at[k], z_recv.at[k],
                      (g, flip(z, k, shards)))

    def arrival(k):
        mask, q = partner(z, k, shards)
        return remote(landed.at[q], out.at[g, z], z_send.at[mask], z_recv.at[mask], (g, q))

    def hop(k, a, h):
        ref = out.at[g, partner(z, k, shards)[1], pl.ds(h * half, half)]
        held = late_y if a else late_x
        target = held.at[late.index(k)] if k in late and a == h else ref
        send, recv = (y_send, y_recv) if a else (x_send, x_recv)
        return remote(ref, target, send.at[k, h], recv.at[k, h], (gy if a else gx, z))

    def turn(k, a):
        ref = out.at[gy if a else gx, partner(z, k, shards)[1], pl.ds(a * half, half)]
        send, recv = (v_send, v_recv) if a else (u_send, u_recv)
        return remote(ref, ref, send.at[k], recv.at[k], (gx if a else gy, z))

    def hops(k):
        return [hop(k, a, h) for a, h in ((0, 0), (1, 1), (0, 1), (1, 0))]

    def advance(k):
        arrival(k).wait_recv()
        for copy in hops(k):
            copy.start()

    def relay(k):
        if k not in late:
            for a in (0, 1):
                hop(k, a, a).wait_recv()
                turn(k, a).start()

    for state in states:
        state.wait()
    for h in (0, 1):
        update(0, h * half, half)
        for a in (0, 1):
            hop(0, a, h).start()
    for i, k in enumerate(made):
        onward(k).wait_recv()
        update(k, 0, rows)
        spread(k).start()
        if i == min(3, shards - 2):
            advance(used[1])
    relay(used[0])
    for s in range(2, shards + 1):
        if s < shards:
            advance(used[s])
        relay(used[s - 1])
    for k in range(1, shards):
        tell_zero(k).wait_send()
        onward(k).wait_send()
        spread(k).wait_send()
    for j in range(1, groups):
        tell_group(j).wait_send()
    for k in order:
        for h in (0, 1):
            for d in (0, 1):
                raw(k, h, d).wait_send()
        for a in (0, 1):
            for h in (0, 1):
                hop(k, a, h).wait_send()
                if a != h or k in late:
                    hop(k, a, h).wait_recv()
            if k not in late:
                turn(k, a).wait()


def patch_kernel(groups, shards, tails, weights, late_x, late_y, came_x, came_y, out, sem):
    del weights
    g, z = lax.axis_index("grp"), lax.axis_index("zero")
    gx, gy, diagonal = flip(g, 1, groups), flip(g, 2, groups), flip(g, 3, groups)
    half = late_x.shape[1]
    used, _ = orders(shards)
    moves = []
    for i, (source, origin, h) in enumerate(
        ((late_x, gx, 0), (late_y, gy, 1), (came_x, diagonal, 0), (came_y, diagonal, 1))
    ):
        for t in range(tails):
            q = partner(z, used[shards - tails + t], shards)[1]
            moves.append(pltpu.make_async_copy(
                source.at[t], out.at[origin, q, pl.ds(h * half, half)], sem.at[i, t]))
    for move in moves:
        move.start()
    for move in moves:
        move.wait()


def store_kernel(pieces, *refs):
    count = len(refs) // 2
    sources, targets, sem = refs[:count], refs[count:2 * count], refs[-1]
    copies = []
    for i, (source, target) in enumerate(zip(sources, targets)):
        size = source.shape[0] // pieces
        for j in range(pieces):
            span = pl.ds(j * size, size)
            copies.append(pltpu.make_async_copy(source.at[span], target.at[span], sem.at[i, j]))
    for copy in copies:
        copy.start()
    for copy in copies:
        copy.wait()


def flat_body(replica_grads, master_weights, first_moment, second_moment, max_norm):
    groups = lax.axis_size("grp")
    shards = lax.axis_size("zero")
    rows = master_weights.shape[0]
    width = replica_grads.shape[3]
    tiles = width // LANES
    deep = 2 * tiles
    bf16, f32 = jnp.bfloat16, jnp.float32
    any_space = pl.BlockSpec(memory_space=pl.ANY)
    vmem = pl.BlockSpec(memory_space=pltpu.VMEM)
    dma = pltpu.SemaphoreType.DMA

    def keep(x, *order):
        return with_layout_constraint(x, Layout(major_to_minor=order))

    def flat(x):
        x = x.reshape(x.shape[0], 2, -1, LANES)
        return jnp.swapaxes(keep(x, 0, 2, 1, 3), 1, 2)

    grad = flat(replica_grads[0]).reshape(groups, shards, 2, rows // 2, deep, LANES)
    master, first, second = (
        flat(x).reshape(rows, shards, deep, LANES)
        for x in (master_weights, first_moment, second_moment)
    )

    block = (shards, rows, deep, LANES)
    state = (rows, shards, deep, LANES)
    tails = min(3, shards - 1)
    late = (tails, rows // 2, deep, LANES)
    grant = 4 * shards * rows * deep * LANES + 192 * 1024
    results = pl.pallas_call(
        functools.partial(step_kernel, groups, shards, tails),
        out_shape=(
            *[pltpu.VMEM(state, f32)] * 3,
            pltpu.VMEM((groups,) + block, bf16),
            *[jax.ShapeDtypeStruct(late, bf16)] * 2,
        ),
        in_specs=[pl.BlockSpec(memory_space=pltpu.SMEM)] + [any_space] * 4,
        out_specs=(vmem,) * 4 + (any_space,) * 2,
        scratch_shapes=[
            *[pltpu.VMEM(block, bf16)] * 2,
            pltpu.VMEM((shards, 8, LANES), f32),
            pltpu.VMEM((groups, 8, LANES), f32),
            *[dma((shards, 2, 2))] * 3,
            *[dma((shards, 2))] * 2,
            *[dma((shards,))] * 4,
            *[dma((groups,))] * 2,
            dma((3,)),
            *[dma((shards,))] * 2,
            *[dma((shards, 2))] * 4,
            *[dma((shards,))] * 4,
        ],
        compiler_params=pltpu.CompilerParams(
            collective_id=0, has_side_effects=True, vmem_limit_bytes=grant
        ),
    )(max_norm, grad, master, first, second)

    pieces = 4
    *states, gathered, late_x, late_y = results
    came_x = lax.ppermute(late_x, "grp", [(i, i ^ 2) for i in range(groups)])
    came_y = lax.ppermute(late_y, "grp", [(i, i ^ 1) for i in range(groups)])
    new_master, new_first, new_second = pl.pallas_call(
        functools.partial(store_kernel, pieces),
        out_shape=(
            *[jax.ShapeDtypeStruct(state, f32)] * 3,
        ),
        in_specs=[any_space] * 3,
        out_specs=(any_space,) * 3,
        scratch_shapes=[dma((3, pieces))],
        compiler_params=pltpu.CompilerParams(vmem_limit_bytes=grant),
        cost_estimate=pl.CostEstimate(flops=0, bytes_accessed=8 * 3 * master.size, transcendentals=0),
    )(*states)
    gathered = pl.pallas_call(
        functools.partial(store_kernel, groups),
        out_shape=jax.ShapeDtypeStruct((groups,) + block, bf16),
        in_specs=[any_space],
        out_specs=any_space,
        scratch_shapes=[dma((1, groups))],
        compiler_params=pltpu.CompilerParams(vmem_limit_bytes=grant),
        cost_estimate=pl.CostEstimate(flops=0, bytes_accessed=4 * gathered.size, transcendentals=0),
    )(gathered)
    gathered = pl.pallas_call(
        functools.partial(patch_kernel, groups, shards, tails),
        out_shape=jax.ShapeDtypeStruct((groups,) + block, bf16),
        in_specs=[any_space] * 5,
        out_specs=any_space,
        input_output_aliases={0: 0},
        scratch_shapes=[dma((4, tails))],
        compiler_params=pltpu.CompilerParams(vmem_limit_bytes=grant),
    )(gathered, *[pltpu.with_memory_space_constraint(x, pltpu.VMEM) for x in (late_x, late_y, came_x, came_y)])

    def unflat(x, shape):
        x = x.reshape(shape[0], -1, 2, LANES)
        return keep(jnp.swapaxes(x, 1, 2), 0, 2, 1, 3).reshape(shape)

    shape = master_weights.shape
    return (
        unflat(new_master, shape),
        unflat(new_first, shape),
        unflat(new_second, shape),
        unflat(gathered, replica_grads.shape[1:]),
    )


def body(replica_grads, master_weights, first_moment, second_moment, max_norm):
    groups = lax.axis_size("grp")
    shards = lax.axis_size("zero")
    rows = master_weights.shape[0]
    width = replica_grads.shape[3]
    deep = 2 * width // LANES
    power = shards > 1 and shards & (shards - 1) == 0
    fits = shards * rows * deep * LANES * (2 * groups + 12 + 4) < 63 * 1024 * 1024
    whole = width % LANES == 0 and deep % 8 == 0 and rows % 2 == 0
    run = flat_body if groups == 4 and power and fits and whole else plain_body
    return run(replica_grads, master_weights, first_moment, second_moment, max_norm)


def solution(mesh):
    in_specs = (
        P("grp", None, None, "zero"),
        P(("grp", "zero"), None, None),
        P(("grp", "zero"), None, None),
        P(("grp", "zero"), None, None),
        P(),
    )
    out_specs = (
        P(("grp", "zero"), None, None),
        P(("grp", "zero"), None, None),
        P(("grp", "zero"), None, None),
        P(None, None, "zero"),
    )
    return jax.shard_map(body, mesh=mesh, in_specs=in_specs, out_specs=out_specs, check_vma=False)
```

```python
import functools

import jax
import jax.numpy as jnp
from jax import lax
from jax.experimental import pallas as pl
from jax.experimental.pallas import tpu as pltpu
from jax.experimental.layout import Layout, with_layout_constraint
from jax.sharding import PartitionSpec as P

ADAM_STEP = 10
MESH = pl.DeviceIdType.MESH
LANES = 128

beta_one = 0.9
beta_two = 0.95
learn_rate = 0.02
adam_eps = 1e-08
norm_eps = 1e-06


def adam_update(summed, master, first, second, scale):
    clipped = summed * scale
    new_first = beta_one * first + (1.0 - beta_one) * clipped
    new_second = beta_two * second + (1.0 - beta_two) * clipped * clipped
    correct_one = 1.0 - beta_one**ADAM_STEP
    correct_two = 1.0 - beta_two**ADAM_STEP
    step_size = new_first / correct_one / (jnp.sqrt(new_second / correct_two) + adam_eps)
    new_master = master - learn_rate * step_size
    return (new_master, new_first, new_second)


def plain_body(replica_grads, master_weights, first_moment, second_moment, max_norm):
    groups = lax.axis_size("grp")
    shards = lax.axis_size("zero")
    local_grad = replica_grads[0]
    local_width = local_grad.shape[2]
    rows_dev = master_weights.shape[0]
    full_width = master_weights.shape[2]
    blocks = local_grad.reshape(groups, shards, rows_dev, 2, local_width)
    arrived = lax.all_to_all(
        lax.all_to_all(blocks[None], "grp", split_axis=1, concat_axis=0, tiled=True),
        "zero",
        split_axis=2,
        concat_axis=5,
        tiled=True,
    )
    summed = jnp.sum(arrived.astype(jnp.float32), axis=0)
    summed = summed.reshape(master_weights.shape)
    total = lax.psum(jnp.sum(summed * summed), ("grp", "zero"))
    scale = jnp.minimum(jnp.float32(1.0), max_norm[0] / (jnp.sqrt(total) + norm_eps))
    new_master, new_first, new_second = adam_update(
        summed, master_weights, first_moment, second_moment, scale
    )
    fresh = new_master.astype(jnp.bfloat16).reshape(1, 1, rows_dev, 2, full_width)
    own_tiles = lax.all_to_all(fresh, "zero", split_axis=4, concat_axis=1, tiled=True)
    tiled = lax.all_gather(own_tiles, "grp", axis=0, tiled=True)
    new_weights = tiled.reshape(groups * shards * rows_dev, 2, full_width // shards)
    return (new_master, new_first, new_second, new_weights)


def flip(index, mask, size):
    out = 0
    bit = 1
    while bit < size:
        b = (index // bit) % 2
        out = out + bit * ((1 - b) if mask & bit else b)
        bit *= 2
    return out


def greet(groups, shards, g, z):
    barrier = pltpu.get_barrier_semaphore()
    for k in range(1, shards):
        pl.semaphore_signal(barrier, inc=1, device_id=(g, flip(z, k, shards)), device_id_type=MESH)
    for j in range(1, groups):
        pl.semaphore_signal(barrier, inc=1, device_id=(flip(g, j, groups), z), device_id_type=MESH)
    pl.semaphore_wait(barrier, shards + groups - 2)


def remote(src, dst, send, recv, device):
    return pltpu.make_async_remote_copy(
        src_ref=src, dst_ref=dst, send_sem=send, recv_sem=recv,
        device_id=device, device_id_type=MESH,
    )


def orders(shards):
    used = [k for k in range(shards) if k != 3 or shards == 4]
    used += [3] * (shards > 4)
    made = [k for k in (shards // 2, 2, shards // 2 + 2, 1) if 0 < k < shards]
    made = list(dict.fromkeys(made + used[1:]))
    return used, made


def partner(z, k, shards):
    low, high = shards // 4, shards // 2
    if low < 2 or k < high:
        return k, flip(z, k, shards)
    one, two = (z // low) % 2, (z // high) % 2
    end = 1 - one - two + 2 * one * two
    return (
        k + end * ((k ^ low) - k),
        flip(z, k, shards) * (1 - end) + flip(z, k ^ low, shards) * end,
    )


def step_kernel(groups, shards, tails, limit, grad, master_in, first_in, second_in, master, first, second, out,
                late_x, late_y, sums, landed, zone, gone, f_send, f_recv, load_sem, p_send, p_recv, s_send, s_recv,
                nz_send, nz_recv, ng_send, ng_recv, state_sem, ready_sem, z_send, z_recv, x_send, x_recv, y_send, y_recv,
                u_send, u_recv, v_send, v_recv, l_send, l_recv):
    g, z = lax.axis_index("grp"), lax.axis_index("zero")
    gx, gy, diagonal = flip(g, 1, groups), flip(g, 2, groups), flip(g, 3, groups)
    first_to, second_to = (gx, gy), (gy, gx)
    rows = landed.shape[1]
    half = rows // 2
    order = list(range(shards - 1, -1, -1))
    used, made = orders(shards)
    late = used[shards - tails:]
    near, far, got, pairs = (out.at[i] for i in range(4))
    bf16, f32 = jnp.bfloat16, jnp.float32
    wide = 4
    first_rows = half // 4

    def part(ref, k, h):
        return ref.at[k, pl.ds(h * half, half)]

    def ready(h):
        return pltpu.make_async_copy(grad.at[diagonal, flip(z, order[0], shards), h], part(landed, z, h),
                                     ready_sem.at[h])

    def raw(k, h, d):
        block = diagonal if d else first_to[h]
        source = part(landed, z, h) if d and k == order[0] else grad.at[block, flip(z, k, shards), h]
        return remote(source, part(far if d else near, k, h),
                      f_send.at[k, h, d], f_recv.at[k, h, d], (first_to[h], z))

    def pair(k, h):
        return remote(part(pairs, k, h), part(got, k, h), p_send.at[k, h], p_recv.at[k, h], (second_to[h], z))

    def load(k, h, d):
        block = second_to[h] if d else g
        return pltpu.make_async_copy(grad.at[block, flip(z, k, shards), h], part(pairs if d else sums, k, h),
                                     load_sem.at[k, h, d])

    def onward(k):
        return remote(sums.at[k], landed.at[z], s_send.at[k], s_recv.at[k], (g, flip(z, k, shards)))

    states = [
        pltpu.make_async_copy(src, dst, state_sem.at[i])
        for i, (src, dst) in enumerate(((master_in, master), (first_in, first), (second_in, second)))
    ]

    for h in (0, 1):
        ready(h).start()
    greet(groups, shards, g, z)
    ahead = 2
    for k in order[:ahead]:
        for h in (0, 1):
            if k == order[0]:
                ready(h).wait()
            raw(k, h, 1).start()
    for k in order:
        for d in (1, 0):
            for h in (0, 1):
                load(k, h, d).start()
    for state in states:
        state.start()
    square = jnp.zeros(landed.shape[2:], f32)
    for i in range(shards + 1):
        if i < shards:
            k = order[i]
            for h in (0, 1):
                load(k, h, 1).wait()
                raw(k, h, 1).wait_recv()

                def join(i, carry, k=k, h=h):
                    for j in range(wide):
                        row = h * half + i * wide + j
                        both = pairs[k, row].astype(f32) + far[k, row].astype(f32)
                        pairs[k, row] = both.astype(bf16)
                    return carry

                lax.fori_loop(0, half // wide, join, 0)
                pair(k, h).start()
            for h in (0, 1):
                raw(k, h, 0).start()
            if i + ahead < shards:
                for h in (0, 1):
                    raw(order[i + ahead], h, 1).start()
        if i >= 1:
            k = order[i - 1]
            for h in (0, 1):
                if k == 0:
                    raw(order[0], h, 1).wait_send()
                load(k, h, 0).wait()
                raw(k, h, 0).wait_recv()
                pair(k, h).wait_recv()

                def add(i, acc, k=k, h=h):
                    parts = []
                    for j in range(wide):
                        row = h * half + i * wide + j
                        total = sums[k, row].astype(f32) + near[k, row].astype(f32)
                        total = total + got[k, row].astype(f32)
                        if k:
                            sums[k, row] = total.astype(bf16)
                        else:
                            landed[z, row] = total.astype(bf16)
                        parts.append(total * total)
                    while len(parts) > 1:
                        parts = [sum(parts[i:i + 2]) for i in range(0, len(parts), 2)]
                    return acc + parts[0]

                square = lax.fori_loop(0, half // wide, add, square)
            if k:
                onward(k).start()

    folded = square[0:8]
    for i in range(8, square.shape[0], 8):
        folded = folded + square[i:i + 8]
    zone[0] = folded

    def tell_zero(k):
        return remote(zone.at[0], zone.at[k], nz_send.at[k], nz_recv.at[k], (g, flip(z, k, shards)))

    def tell_group(j):
        return remote(gone.at[0], gone.at[j], ng_send.at[j], ng_recv.at[j], (flip(g, j, groups), z))

    for k in order:
        for h in (0, 1):
            pair(k, h).wait_send()
    for k in range(1, shards):
        tell_zero(k).start()
    for k in range(1, shards):
        tell_zero(k).wait_recv()
    gone[0] = jnp.sum(zone[...], axis=0)
    for j in range(1, groups):
        tell_group(j).start()
    for j in range(1, groups):
        tell_group(j).wait_recv()
    norm = jnp.sum(gone[...], axis=0)
    total = jnp.full(landed.shape[2:], jnp.sum(norm), f32)
    scale = jnp.minimum(f32(1.0), limit[0] / (jnp.sqrt(total) + norm_eps))
    rate_one = learn_rate / (1.0 - beta_one**ADAM_STEP)
    over_two = 1.0 / (1.0 - beta_two**ADAM_STEP)

    def update(k, start, count):
        c = flip(z, k, shards)

        def some(i, carry):
            for j in range(wide):
                r = start + i * wide + j
                clipped = landed[c, r].astype(f32) * scale
                new_first = beta_one * first[r, c] + (1.0 - beta_one) * clipped
                new_second = beta_two * second[r, c] + (1.0 - beta_two) * clipped * clipped
                below = jnp.sqrt(new_second * over_two) + adam_eps
                new_master = master[r, c] - new_first * rate_one / below
                master[r, c] = new_master
                first[r, c] = new_first
                second[r, c] = new_second
                if k:
                    landed[c, r] = new_master.astype(bf16)
                else:
                    out[g, z, r] = new_master.astype(bf16)
            return carry

        lax.fori_loop(0, count // wide, some, 0)

    def spread(k):
        return remote(landed.at[flip(z, k, shards)], out.at[g, z], z_send.at[k], z_recv.at[k],
                      (g, flip(z, k, shards)))

    def arrival(k):
        mask, q = partner(z, k, shards)
        return remote(landed.at[q], out.at[g, z], z_send.at[mask], z_recv.at[mask], (g, q))

    def hop(k, a, h):
        skip = first_rows if k == 0 and h == 0 else 0
        ref = out.at[g, partner(z, k, shards)[1], pl.ds(h * half + skip, half - skip)]
        held = late_y if a else late_x
        target = held.at[late.index(k)] if k in late and a == h else ref
        send, recv = (y_send, y_recv) if a else (x_send, x_recv)
        return remote(ref, target, send.at[k, h], recv.at[k, h], (gy if a else gx, z))

    def lead(a):
        ref = out.at[g, z, pl.ds(0, first_rows)]
        return remote(ref, ref, l_send.at[a], l_recv.at[a], (gy if a else gx, z))

    def turn(k, a):
        ref = out.at[gy if a else gx, partner(z, k, shards)[1], pl.ds(a * half, half)]
        send, recv = (v_send, v_recv) if a else (u_send, u_recv)
        return remote(ref, ref, send.at[k], recv.at[k], (gx if a else gy, z))

    def hops(k):
        return [hop(k, a, h) for a, h in ((0, 0), (1, 1), (0, 1), (1, 0))]

    def advance(k):
        arrival(k).wait_recv()
        for copy in hops(k):
            copy.start()

    def finish(k):
        if k:
            spread(k).wait_send()
        for a in (0, 1):
            for h in (0, 1):
                hop(k, a, h).wait_send()
                if a != h or k in late:
                    hop(k, a, h).wait_recv()
            if k == 0:
                lead(a).wait_send()
                if a:
                    lead(a).wait_recv()
            if k not in late:
                turn(k, a).wait()

    def relay(k):
        if k not in late:
            for a in (0, 1):
                hop(k, a, a).wait_recv()
                if k == 0 and a == 0:
                    lead(a).wait_recv()
                turn(k, a).start()

    for state in states:
        state.wait()
    update(0, 0, first_rows)
    for a in (0, 1):
        lead(a).start()
    for h, skip in ((0, first_rows), (1, 0)):
        update(0, h * half + skip, half - skip)
        for a in (0, 1):
            hop(0, a, h).start()
    for i, k in enumerate(made):
        onward(k).wait_recv()
        update(k, 0, rows)
        spread(k).start()
        if i == 3:
            advance(used[1])
    for k in range(1, shards):
        tell_zero(k).wait_send()
        onward(k).wait_send()
    for j in range(1, groups):
        tell_group(j).wait_send()
    for k in order:
        for h in (0, 1):
            for d in (0, 1):
                if d == 0 or k != order[0]:
                    raw(k, h, d).wait_send()
    relay(used[0])
    for s in range(2, shards + 1):
        if s < shards:
            advance(used[s])
        relay(used[s - 1])
        if s >= 4:
            finish(used[s - 4])
    for k in used[shards - 3:]:
        finish(k)


def late_moves(groups, shards, tails, sources, origins, out, sem):
    z = lax.axis_index("zero")
    used, _ = orders(shards)
    half = out.shape[2] // 2
    moves = []
    for h in (0, 1):
        for t in range(tails):
            q = partner(z, used[shards - tails + t], shards)[1]
            moves.append(pltpu.make_async_copy(
                sources[h].at[t], out.at[origins[h], q, pl.ds(h * half, half)], sem.at[h, t]))
    return moves


def weight_kernel(groups, shards, tails, gathered, late_x, late_y, out, hold_x, hold_y, load_sem, sem, late_sem):
    g = lax.axis_index("grp")
    origins = (flip(g, 1, groups), flip(g, 2, groups))
    loads = [
        pltpu.make_async_copy(late_x, hold_x, load_sem.at[0]),
        pltpu.make_async_copy(late_y, hold_y, load_sem.at[1]),
    ]
    copies = [pltpu.make_async_copy(gathered.at[i], out.at[i], sem.at[i]) for i in range(groups)]
    moves = late_moves(groups, shards, tails, (hold_x, hold_y), origins, out, late_sem)
    for copy in loads + copies:
        copy.start()
    for copy in loads + copies:
        copy.wait()
    for copy in moves:
        copy.start()
    for copy in moves:
        copy.wait()


def patch_kernel(groups, shards, tails, weights, came_x, came_y, out, sem):
    del weights
    diagonal = flip(lax.axis_index("grp"), 3, groups)
    moves = late_moves(groups, shards, tails, (came_x, came_y), (diagonal, diagonal), out, sem)
    for move in moves:
        move.start()
    for move in moves:
        move.wait()


def store_kernel(pieces, *refs):
    count = len(refs) // 2
    sources, targets, sem = refs[:count], refs[count:2 * count], refs[-1]
    copies = []
    for i, (source, target) in enumerate(zip(sources, targets)):
        size = source.shape[0] // pieces
        for j in range(pieces):
            span = pl.ds(j * size, size)
            copies.append(pltpu.make_async_copy(source.at[span], target.at[span], sem.at[i, j]))
    for copy in copies:
        copy.start()
    for copy in copies:
        copy.wait()


def flat_body(replica_grads, master_weights, first_moment, second_moment, max_norm):
    groups = lax.axis_size("grp")
    shards = lax.axis_size("zero")
    rows = master_weights.shape[0]
    width = replica_grads.shape[3]
    tiles = width // LANES
    deep = 2 * tiles
    bf16, f32 = jnp.bfloat16, jnp.float32
    any_space = pl.BlockSpec(memory_space=pl.ANY)
    vmem = pl.BlockSpec(memory_space=pltpu.VMEM)
    dma = pltpu.SemaphoreType.DMA

    def keep(x, *order):
        return with_layout_constraint(x, Layout(major_to_minor=order))

    def flat(x):
        x = x.reshape(x.shape[0], 2, -1, LANES)
        return jnp.swapaxes(keep(x, 0, 2, 1, 3), 1, 2)

    grad = flat(replica_grads[0]).reshape(groups, shards, 2, rows // 2, deep, LANES)
    master, first, second = (
        flat(x).reshape(rows, shards, deep, LANES)
        for x in (master_weights, first_moment, second_moment)
    )

    block = (shards, rows, deep, LANES)
    state = (rows, shards, deep, LANES)
    tails = 3
    late = (tails, rows // 2, deep, LANES)
    grant = 4 * shards * rows * deep * LANES + 192 * 1024
    results = pl.pallas_call(
        functools.partial(step_kernel, groups, shards, tails),
        out_shape=(
            *[pltpu.VMEM(state, f32)] * 3,
            pltpu.VMEM((groups,) + block, bf16),
            *[jax.ShapeDtypeStruct(late, bf16)] * 2,
        ),
        in_specs=[pl.BlockSpec(memory_space=pltpu.SMEM)] + [any_space] * 4,
        out_specs=(vmem,) * 4 + (any_space,) * 2,
        scratch_shapes=[
            *[pltpu.VMEM(block, bf16)] * 2,
            pltpu.VMEM((shards, 8, LANES), f32),
            pltpu.VMEM((groups, 8, LANES), f32),
            *[dma((shards, 2, 2))] * 3,
            *[dma((shards, 2))] * 2,
            *[dma((shards,))] * 4,
            *[dma((groups,))] * 2,
            dma((3,)),
            dma((2,)),
            *[dma((shards,))] * 2,
            *[dma((shards, 2))] * 4,
            *[dma((shards,))] * 4,
            *[dma((2,))] * 2,
        ],
        compiler_params=pltpu.CompilerParams(
            collective_id=0, has_side_effects=True, vmem_limit_bytes=grant
        ),
    )(max_norm, grad, master, first, second)

    pieces = 4
    *states, gathered, late_x, late_y = results
    came_x = lax.ppermute(late_x, "grp", [(i, i ^ 2) for i in range(groups)])
    came_y = lax.ppermute(late_y, "grp", [(i, i ^ 1) for i in range(groups)])
    new_master, new_first, new_second = pl.pallas_call(
        functools.partial(store_kernel, pieces),
        out_shape=(
            *[jax.ShapeDtypeStruct(state, f32)] * 3,
        ),
        in_specs=[any_space] * 3,
        out_specs=(any_space,) * 3,
        scratch_shapes=[dma((3, pieces))],
        compiler_params=pltpu.CompilerParams(vmem_limit_bytes=grant),
        cost_estimate=pl.CostEstimate(flops=0, bytes_accessed=8 * 3 * master.size, transcendentals=0),
    )(*states)
    gathered = pl.pallas_call(
        functools.partial(weight_kernel, groups, shards, tails),
        out_shape=jax.ShapeDtypeStruct((groups,) + block, bf16),
        in_specs=[any_space] * 3,
        out_specs=any_space,
        scratch_shapes=[*[pltpu.VMEM(late, bf16)] * 2, dma((2,)), dma((groups,)), dma((2, tails))],
        compiler_params=pltpu.CompilerParams(vmem_limit_bytes=grant),
        cost_estimate=pl.CostEstimate(flops=0, bytes_accessed=4 * gathered.size, transcendentals=0),
    )(gathered, *[pltpu.with_memory_space_constraint(x, pltpu.HBM) for x in (late_x, late_y)])
    gathered = pl.pallas_call(
        functools.partial(patch_kernel, groups, shards, tails),
        out_shape=jax.ShapeDtypeStruct((groups,) + block, bf16),
        in_specs=[any_space] * 3,
        out_specs=any_space,
        input_output_aliases={0: 0},
        scratch_shapes=[dma((2, tails))],
        compiler_params=pltpu.CompilerParams(vmem_limit_bytes=grant),
    )(gathered, *[pltpu.with_memory_space_constraint(x, pltpu.VMEM) for x in (came_x, came_y)])

    def unflat(x, shape):
        x = x.reshape(shape[0], -1, 2, LANES)
        return keep(jnp.swapaxes(x, 1, 2), 0, 2, 1, 3).reshape(shape)

    shape = master_weights.shape
    return (
        unflat(new_master, shape),
        unflat(new_first, shape),
        unflat(new_second, shape),
        unflat(gathered, replica_grads.shape[1:]),
    )


def body(replica_grads, master_weights, first_moment, second_moment, max_norm):
    groups = lax.axis_size("grp")
    shards = lax.axis_size("zero")
    rows = master_weights.shape[0]
    width = replica_grads.shape[3]
    deep = 2 * width // LANES
    power = shards >= 8 and shards & (shards - 1) == 0
    fits = shards * rows * deep * LANES * (2 * groups + 12 + 4) < 63 * 1024 * 1024
    whole = width % LANES == 0 and deep % 8 == 0 and rows % 32 == 0
    run = flat_body if groups == 4 and power and fits and whole else plain_body
    return run(replica_grads, master_weights, first_moment, second_moment, max_norm)


def solution(mesh):
    in_specs = (
        P("grp", None, None, "zero"),
        P(("grp", "zero"), None, None),
        P(("grp", "zero"), None, None),
        P(("grp", "zero"), None, None),
        P(),
    )
    out_specs = (
        P(("grp", "zero"), None, None),
        P(("grp", "zero"), None, None),
        P(("grp", "zero"), None, None),
        P(None, None, "zero"),
    )
    return jax.shard_map(body, mesh=mesh, in_specs=in_specs, out_specs=out_specs, check_vma=False)
```

```python
import functools

import jax
import jax.numpy as jnp
from jax import lax
from jax.experimental import pallas as pl
from jax.experimental.pallas import tpu as pltpu
from jax.experimental.layout import Layout, with_layout_constraint
from jax.sharding import PartitionSpec as P

ADAM_STEP = 10
MESH = pl.DeviceIdType.MESH
LANES = 128

beta_one = 0.9
beta_two = 0.95
learn_rate = 0.02
adam_eps = 1e-08
norm_eps = 1e-06


def adam_update(summed, master, first, second, scale):
    clipped = summed * scale
    new_first = beta_one * first + (1.0 - beta_one) * clipped
    new_second = beta_two * second + (1.0 - beta_two) * clipped * clipped
    correct_one = 1.0 - beta_one**ADAM_STEP
    correct_two = 1.0 - beta_two**ADAM_STEP
    step_size = new_first / correct_one / (jnp.sqrt(new_second / correct_two) + adam_eps)
    new_master = master - learn_rate * step_size
    return (new_master, new_first, new_second)


def plain_body(replica_grads, master_weights, first_moment, second_moment, max_norm):
    groups = lax.axis_size("grp")
    shards = lax.axis_size("zero")
    local_grad = replica_grads[0]
    local_width = local_grad.shape[2]
    rows_dev = master_weights.shape[0]
    full_width = master_weights.shape[2]
    blocks = local_grad.reshape(groups, shards, rows_dev, 2, local_width)
    arrived = lax.all_to_all(
        lax.all_to_all(blocks[None], "grp", split_axis=1, concat_axis=0, tiled=True),
        "zero",
        split_axis=2,
        concat_axis=5,
        tiled=True,
    )
    summed = jnp.sum(arrived.astype(jnp.float32), axis=0)
    summed = summed.reshape(master_weights.shape)
    total = lax.psum(jnp.sum(summed * summed), ("grp", "zero"))
    scale = jnp.minimum(jnp.float32(1.0), max_norm[0] / (jnp.sqrt(total) + norm_eps))
    new_master, new_first, new_second = adam_update(
        summed, master_weights, first_moment, second_moment, scale
    )
    fresh = new_master.astype(jnp.bfloat16).reshape(1, 1, rows_dev, 2, full_width)
    own_tiles = lax.all_to_all(fresh, "zero", split_axis=4, concat_axis=1, tiled=True)
    tiled = lax.all_gather(own_tiles, "grp", axis=0, tiled=True)
    new_weights = tiled.reshape(groups * shards * rows_dev, 2, full_width // shards)
    return (new_master, new_first, new_second, new_weights)


def flip(index, mask, size):
    out = 0
    bit = 1
    while bit < size:
        b = (index // bit) % 2
        out = out + bit * ((1 - b) if mask & bit else b)
        bit *= 2
    return out


def greet(groups, shards, g, z):
    barrier = pltpu.get_barrier_semaphore()
    for k in range(1, shards):
        pl.semaphore_signal(barrier, inc=1, device_id=(g, flip(z, k, shards)), device_id_type=MESH)
    for j in range(1, groups):
        pl.semaphore_signal(barrier, inc=1, device_id=(flip(g, j, groups), z), device_id_type=MESH)
    pl.semaphore_wait(barrier, shards + groups - 2)


def remote(src, dst, send, recv, device):
    return pltpu.make_async_remote_copy(
        src_ref=src, dst_ref=dst, send_sem=send, recv_sem=recv,
        device_id=device, device_id_type=MESH,
    )


def orders(shards):
    used = [k for k in range(shards) if k != 3 or shards == 4]
    used += [3] * (shards > 4)
    made = [k for k in (shards // 2, 2, shards // 2 + 2, 1) if 0 < k < shards]
    made = list(dict.fromkeys(made + used[1:]))
    return used, made


def partner(z, k, shards):
    low, high = shards // 4, shards // 2
    if low < 2 or k < high:
        return k, flip(z, k, shards)
    one, two = (z // low) % 2, (z // high) % 2
    end = 1 - one - two + 2 * one * two
    return (
        k + end * ((k ^ low) - k),
        flip(z, k, shards) * (1 - end) + flip(z, k ^ low, shards) * end,
    )


def step_kernel(groups, shards, tails, limit, grad, master_in, first_in, second_in, master, first, second, out,
                late_x, late_y, sums, landed, zone, gone, f_send, f_recv, load_sem, p_send, p_recv, s_send, s_recv,
                nz_send, nz_recv, ng_send, ng_recv, state_sem, ready_sem, z_send, z_recv, x_send, x_recv, y_send, y_recv,
                u_send, u_recv, v_send, v_recv, l_send, l_recv):
    g, z = lax.axis_index("grp"), lax.axis_index("zero")
    gx, gy, diagonal = flip(g, 1, groups), flip(g, 2, groups), flip(g, 3, groups)
    first_to, second_to = (gx, gy), (gy, gx)
    rows = landed.shape[1]
    half = rows // 2
    order = list(range(shards - 1, -1, -1))
    used, made = orders(shards)
    late = used[shards - tails:]
    near, far, got, pairs = (out.at[i] for i in range(4))
    bf16, f32 = jnp.bfloat16, jnp.float32
    wide = 4
    first_rows = half // 4

    def part(ref, k, h):
        return ref.at[k, pl.ds(h * half, half)]

    def ready(h):
        return pltpu.make_async_copy(grad.at[diagonal, flip(z, order[0], shards), h], part(landed, z, h),
                                     ready_sem.at[h])

    def raw(k, h, d):
        block = diagonal if d else first_to[h]
        source = part(landed, z, h) if d and k == order[0] else grad.at[block, flip(z, k, shards), h]
        return remote(source, part(far if d else near, k, h),
                      f_send.at[k, h, d], f_recv.at[k, h, d], (first_to[h], z))

    def pair(k, h):
        return remote(part(pairs, k, h), part(got, k, h), p_send.at[k, h], p_recv.at[k, h], (second_to[h], z))

    def load(k, h, d):
        block = second_to[h] if d else g
        return pltpu.make_async_copy(grad.at[block, flip(z, k, shards), h], part(pairs if d else sums, k, h),
                                     load_sem.at[k, h, d])

    def onward(k):
        return remote(sums.at[k], landed.at[z], s_send.at[k], s_recv.at[k], (g, flip(z, k, shards)))

    states = [
        pltpu.make_async_copy(src, dst, state_sem.at[i])
        for i, (src, dst) in enumerate(((master_in, master), (first_in, first), (second_in, second)))
    ]

    for h in (0, 1):
        ready(h).start()
    greet(groups, shards, g, z)
    ahead = 2
    for k in order[:ahead]:
        for h in (0, 1):
            if k == order[0]:
                ready(h).wait()
            raw(k, h, 1).start()
    for k in order:
        for d in (1, 0):
            for h in (0, 1):
                load(k, h, d).start()
    for state in states:
        state.start()
    square = jnp.zeros(landed.shape[2:], f32)
    for i in range(shards + 1):
        if i < shards:
            k = order[i]
            for h in (0, 1):
                raw(k, h, 0).start()
            for h in (0, 1):
                load(k, h, 1).wait()
                raw(k, h, 1).wait_recv()

                def join(i, carry, k=k, h=h):
                    for j in range(wide):
                        row = h * half + i * wide + j
                        both = pairs[k, row].astype(f32) + far[k, row].astype(f32)
                        pairs[k, row] = both.astype(bf16)
                    return carry

                lax.fori_loop(0, half // wide, join, 0)
                pair(k, h).start()
            if i + ahead < shards:
                for h in (0, 1):
                    raw(order[i + ahead], h, 1).start()
        if i >= 1:
            k = order[i - 1]
            for h in (0, 1):
                if k == 0:
                    raw(order[0], h, 1).wait_send()
                load(k, h, 0).wait()
                raw(k, h, 0).wait_recv()
                pair(k, h).wait_recv()

                def add(i, acc, k=k, h=h):
                    parts = []
                    for j in range(wide):
                        row = h * half + i * wide + j
                        total = sums[k, row].astype(f32) + near[k, row].astype(f32)
                        total = total + got[k, row].astype(f32)
                        if k:
                            sums[k, row] = total.astype(bf16)
                        else:
                            landed[z, row] = total.astype(bf16)
                        parts.append(total * total)
                    while len(parts) > 1:
                        parts = [sum(parts[i:i + 2]) for i in range(0, len(parts), 2)]
                    return acc + parts[0]

                square = lax.fori_loop(0, half // wide, add, square)
            if k:
                onward(k).start()

    folded = square[0:8]
    for i in range(8, square.shape[0], 8):
        folded = folded + square[i:i + 8]
    zone[0] = folded

    def tell_zero(k):
        return remote(zone.at[0], zone.at[k], nz_send.at[k], nz_recv.at[k], (g, flip(z, k, shards)))

    def tell_group(j):
        return remote(gone.at[0], gone.at[j], ng_send.at[j], ng_recv.at[j], (flip(g, j, groups), z))

    for k in order:
        for h in (0, 1):
            pair(k, h).wait_send()
    for k in range(1, shards):
        tell_zero(k).start()
    for k in range(1, shards):
        tell_zero(k).wait_recv()
    gone[0] = jnp.sum(zone[...], axis=0)
    for j in range(1, groups):
        tell_group(j).start()
    for j in range(1, groups):
        tell_group(j).wait_recv()
    norm = jnp.sum(gone[...], axis=0)
    total = jnp.full(landed.shape[2:], jnp.sum(norm), f32)
    scale = jnp.minimum(f32(1.0), limit[0] / (jnp.sqrt(total) + norm_eps))
    rate_one = learn_rate / (1.0 - beta_one**ADAM_STEP)
    over_two = 1.0 / (1.0 - beta_two**ADAM_STEP)

    def update(k, start, count):
        c = flip(z, k, shards)

        def some(i, carry):
            for j in range(wide):
                r = start + i * wide + j
                clipped = landed[c, r].astype(f32) * scale
                new_first = beta_one * first[r, c] + (1.0 - beta_one) * clipped
                new_second = beta_two * second[r, c] + (1.0 - beta_two) * clipped * clipped
                below = jnp.sqrt(new_second * over_two) + adam_eps
                new_master = master[r, c] - new_first * rate_one / below
                master[r, c] = new_master
                first[r, c] = new_first
                second[r, c] = new_second
                if k:
                    landed[c, r] = new_master.astype(bf16)
                else:
                    out[g, z, r] = new_master.astype(bf16)
            return carry

        lax.fori_loop(0, count // wide, some, 0)

    def spread(k):
        return remote(landed.at[flip(z, k, shards)], out.at[g, z], z_send.at[k], z_recv.at[k],
                      (g, flip(z, k, shards)))

    def arrival(k):
        mask, q = partner(z, k, shards)
        return remote(landed.at[q], out.at[g, z], z_send.at[mask], z_recv.at[mask], (g, q))

    def hop(k, a, h):
        skip = first_rows if k == 0 and h == 0 else 0
        ref = out.at[g, partner(z, k, shards)[1], pl.ds(h * half + skip, half - skip)]
        held = late_y if a else late_x
        target = held.at[late.index(k)] if k in late and a == h else ref
        send, recv = (y_send, y_recv) if a else (x_send, x_recv)
        return remote(ref, target, send.at[k, h], recv.at[k, h], (gy if a else gx, z))

    def lead(a):
        ref = out.at[g, z, pl.ds(0, first_rows)]
        return remote(ref, ref, l_send.at[a], l_recv.at[a], (gy if a else gx, z))

    def turn(k, a):
        ref = out.at[gy if a else gx, partner(z, k, shards)[1], pl.ds(a * half, half)]
        send, recv = (v_send, v_recv) if a else (u_send, u_recv)
        return remote(ref, ref, send.at[k], recv.at[k], (gx if a else gy, z))

    def hops(k):
        return [hop(k, a, h) for a, h in ((0, 0), (1, 1), (0, 1), (1, 0))]

    def advance(k):
        arrival(k).wait_recv()
        for copy in hops(k):
            copy.start()

    def finish(k):
        if k:
            spread(k).wait_send()
        for a in (0, 1):
            for h in (0, 1):
                hop(k, a, h).wait_send()
                if a != h or k in late:
                    hop(k, a, h).wait_recv()
            if k == 0:
                lead(a).wait_send()
                if a:
                    lead(a).wait_recv()
            if k not in late:
                turn(k, a).wait()

    def relay(k):
        if k not in late:
            for a in (0, 1):
                hop(k, a, a).wait_recv()
                if k == 0 and a == 0:
                    lead(a).wait_recv()
                turn(k, a).start()

    for state in states:
        state.wait()
    update(0, 0, first_rows)
    for a in (0, 1):
        lead(a).start()
    for h, skip in ((0, first_rows), (1, 0)):
        update(0, h * half + skip, half - skip)
        for a in (0, 1):
            hop(0, a, h).start()
    for i, k in enumerate(made):
        onward(k).wait_recv()
        update(k, 0, rows)
        spread(k).start()
        if i == 3:
            advance(used[1])
    for k in range(1, shards):
        tell_zero(k).wait_send()
        onward(k).wait_send()
    for j in range(1, groups):
        tell_group(j).wait_send()
    for k in order:
        for h in (0, 1):
            for d in (0, 1):
                if d == 0 or k != order[0]:
                    raw(k, h, d).wait_send()
    relay(used[0])
    for s in range(2, shards + 1):
        if s < shards:
            advance(used[s])
        relay(used[s - 1])
        if s >= 4:
            finish(used[s - 4])
    for k in used[shards - 3:]:
        finish(k)


def late_moves(groups, shards, tails, sources, origins, out, sem):
    z = lax.axis_index("zero")
    used, _ = orders(shards)
    half = out.shape[2] // 2
    moves = []
    for h in (0, 1):
        for t in range(tails):
            q = partner(z, used[shards - tails + t], shards)[1]
            moves.append(pltpu.make_async_copy(
                sources[h].at[t], out.at[origins[h], q, pl.ds(h * half, half)], sem.at[h, t]))
    return moves


def weight_kernel(groups, shards, tails, gathered, late_x, late_y, out, hold_x, hold_y, load_sem, sem, late_sem):
    g = lax.axis_index("grp")
    origins = (flip(g, 1, groups), flip(g, 2, groups))
    loads = [
        pltpu.make_async_copy(late_x, hold_x, load_sem.at[0]),
        pltpu.make_async_copy(late_y, hold_y, load_sem.at[1]),
    ]
    copies = [pltpu.make_async_copy(gathered.at[i], out.at[i], sem.at[i]) for i in range(groups)]
    moves = late_moves(groups, shards, tails, (hold_x, hold_y), origins, out, late_sem)
    for copy in loads + copies:
        copy.start()
    for copy in loads + copies:
        copy.wait()
    for copy in moves:
        copy.start()
    for copy in moves:
        copy.wait()


def patch_kernel(groups, shards, tails, weights, came_x, came_y, out, sem):
    del weights
    diagonal = flip(lax.axis_index("grp"), 3, groups)
    moves = late_moves(groups, shards, tails, (came_x, came_y), (diagonal, diagonal), out, sem)
    for move in moves:
        move.start()
    for move in moves:
        move.wait()


def store_kernel(pieces, *refs):
    count = len(refs) // 2
    sources, targets, sem = refs[:count], refs[count:2 * count], refs[-1]
    copies = []
    for i, (source, target) in enumerate(zip(sources, targets)):
        size = source.shape[0] // pieces
        for j in range(pieces):
            span = pl.ds(j * size, size)
            copies.append(pltpu.make_async_copy(source.at[span], target.at[span], sem.at[i, j]))
    for copy in copies:
        copy.start()
    for copy in copies:
        copy.wait()


def flat_body(replica_grads, master_weights, first_moment, second_moment, max_norm):
    groups = lax.axis_size("grp")
    shards = lax.axis_size("zero")
    rows = master_weights.shape[0]
    width = replica_grads.shape[3]
    tiles = width // LANES
    deep = 2 * tiles
    bf16, f32 = jnp.bfloat16, jnp.float32
    any_space = pl.BlockSpec(memory_space=pl.ANY)
    vmem = pl.BlockSpec(memory_space=pltpu.VMEM)
    dma = pltpu.SemaphoreType.DMA

    def keep(x, *order):
        return with_layout_constraint(x, Layout(major_to_minor=order))

    def flat(x):
        x = x.reshape(x.shape[0], 2, -1, LANES)
        return jnp.swapaxes(keep(x, 0, 2, 1, 3), 1, 2)

    grad = flat(replica_grads[0]).reshape(groups, shards, 2, rows // 2, deep, LANES)
    master, first, second = (
        flat(x).reshape(rows, shards, deep, LANES)
        for x in (master_weights, first_moment, second_moment)
    )

    block = (shards, rows, deep, LANES)
    state = (rows, shards, deep, LANES)
    tails = 3
    late = (tails, rows // 2, deep, LANES)
    grant = 4 * shards * rows * deep * LANES + 192 * 1024
    results = pl.pallas_call(
        functools.partial(step_kernel, groups, shards, tails),
        out_shape=(
            *[pltpu.VMEM(state, f32)] * 3,
            pltpu.VMEM((groups,) + block, bf16),
            *[jax.ShapeDtypeStruct(late, bf16)] * 2,
        ),
        in_specs=[pl.BlockSpec(memory_space=pltpu.SMEM)] + [any_space] * 4,
        out_specs=(vmem,) * 4 + (any_space,) * 2,
        scratch_shapes=[
            *[pltpu.VMEM(block, bf16)] * 2,
            pltpu.VMEM((shards, 8, LANES), f32),
            pltpu.VMEM((groups, 8, LANES), f32),
            *[dma((shards, 2, 2))] * 3,
            *[dma((shards, 2))] * 2,
            *[dma((shards,))] * 4,
            *[dma((groups,))] * 2,
            dma((3,)),
            dma((2,)),
            *[dma((shards,))] * 2,
            *[dma((shards, 2))] * 4,
            *[dma((shards,))] * 4,
            *[dma((2,))] * 2,
        ],
        compiler_params=pltpu.CompilerParams(
            collective_id=0, has_side_effects=True, vmem_limit_bytes=grant
        ),
    )(max_norm, grad, master, first, second)

    pieces = 4
    *states, gathered, late_x, late_y = results
    came_x = lax.ppermute(late_x, "grp", [(i, i ^ 2) for i in range(groups)])
    came_y = lax.ppermute(late_y, "grp", [(i, i ^ 1) for i in range(groups)])
    new_master, new_first, new_second = pl.pallas_call(
        functools.partial(store_kernel, pieces),
        out_shape=(
            *[jax.ShapeDtypeStruct(state, f32)] * 3,
        ),
        in_specs=[any_space] * 3,
        out_specs=(any_space,) * 3,
        scratch_shapes=[dma((3, pieces))],
        compiler_params=pltpu.CompilerParams(vmem_limit_bytes=grant),
        cost_estimate=pl.CostEstimate(flops=0, bytes_accessed=8 * 3 * master.size, transcendentals=0),
    )(*states)
    gathered = pl.pallas_call(
        functools.partial(weight_kernel, groups, shards, tails),
        out_shape=jax.ShapeDtypeStruct((groups,) + block, bf16),
        in_specs=[any_space] * 3,
        out_specs=any_space,
        scratch_shapes=[*[pltpu.VMEM(late, bf16)] * 2, dma((2,)), dma((groups,)), dma((2, tails))],
        compiler_params=pltpu.CompilerParams(vmem_limit_bytes=grant),
        cost_estimate=pl.CostEstimate(flops=0, bytes_accessed=4 * gathered.size, transcendentals=0),
    )(gathered, *[pltpu.with_memory_space_constraint(x, pltpu.HBM) for x in (late_x, late_y)])
    gathered = pl.pallas_call(
        functools.partial(patch_kernel, groups, shards, tails),
        out_shape=jax.ShapeDtypeStruct((groups,) + block, bf16),
        in_specs=[any_space] * 3,
        out_specs=any_space,
        input_output_aliases={0: 0},
        scratch_shapes=[dma((2, tails))],
        compiler_params=pltpu.CompilerParams(vmem_limit_bytes=grant),
    )(gathered, *[pltpu.with_memory_space_constraint(x, pltpu.VMEM) for x in (came_x, came_y)])

    def unflat(x, shape):
        x = x.reshape(shape[0], -1, 2, LANES)
        return keep(jnp.swapaxes(x, 1, 2), 0, 2, 1, 3).reshape(shape)

    shape = master_weights.shape
    return (
        unflat(new_master, shape),
        unflat(new_first, shape),
        unflat(new_second, shape),
        unflat(gathered, replica_grads.shape[1:]),
    )


def body(replica_grads, master_weights, first_moment, second_moment, max_norm):
    groups = lax.axis_size("grp")
    shards = lax.axis_size("zero")
    rows = master_weights.shape[0]
    width = replica_grads.shape[3]
    deep = 2 * width // LANES
    power = shards >= 8 and shards & (shards - 1) == 0
    fits = shards * rows * deep * LANES * (2 * groups + 12 + 4) < 63 * 1024 * 1024
    whole = width % LANES == 0 and deep % 8 == 0 and rows % 32 == 0
    run = flat_body if groups == 4 and power and fits and whole else plain_body
    return run(replica_grads, master_weights, first_moment, second_moment, max_norm)


def solution(mesh):
    in_specs = (
        P("grp", None, None, "zero"),
        P(("grp", "zero"), None, None),
        P(("grp", "zero"), None, None),
        P(("grp", "zero"), None, None),
        P(),
    )
    out_specs = (
        P(("grp", "zero"), None, None),
        P(("grp", "zero"), None, None),
        P(("grp", "zero"), None, None),
        P(None, None, "zero"),
    )
    return jax.shard_map(body, mesh=mesh, in_specs=in_specs, out_specs=out_specs, check_vma=False)
```
